32 devices in a mesh: pair: 8 (over y, x, core), aux: 4 (over z).
Axes of the slice: x: 2, y: 2, z: 4, core: 2. Of those that a mesh axis runs over, the one named last changes fastest.
Arguments:
- integrals: bfloat16 [512, 256, 64], P(('pair', 'aux')), may hold values from -6 to 6
- amplitudes: bfloat16 [512, 64, 64], P(('pair', 'aux')), may hold values from -0.75 to 0.75
- pno_density: bfloat16 [512, 64, 64], P(('pair', 'aux')), may hold values from -6 to 6
- pno_coef: bfloat16 [512, 256, 64], P(('pair', 'aux')), may hold values from -0.75 to 0.75
- pao_blocks: int32 [512, 2], P(('pair', 'aux')), may hold values from 0 to 5, all different within a row
- aux_slice: int32 [512, 2], P(('pair', 'aux')), may hold values from 0 to 3, all different within a row; in each aligned block of 16 rows (0 to 15, 16 to 31, ...) at most 16 rows name the same one
- aux_offset: int32 [512, 2], P(('pair', 'aux')), may hold values from 0 to 3
Outputs:
- aux_density: float32 [2048, 768], P('aux', 'pair')
- virtual_density: float32 [768, 768], P('aux', 'pair')
The draws below stay inside these ranges and needn't reach their ends.
Inputs may be any that keep to these rules, and one draw needn't show every extreme that they name: `pao_blocks`: the 2 blocks of a pair are different. `aux_slice`: the 2 slices of a pair are different; among the pairs of one device no slice is named more than 16 times, and in every draw some device names some slice exactly 16 times.
All inputs are finite; a program needn't handle non-finite values.
Results may differ from the reference program's by a relative error of at most 0.0041.
Values may be sent and summed in bfloat16 or wider, within the bound.
A program may use at most 64 MiB of HBM per device.

```python
import math
import jax
import jax.numpy as jnp
import numpy as np
from jax import lax

NPNO = 64
ABLK = 128
PBLK = 128
DOMB = 2
ADOM = 2
NBLK = 6
ABPO = 4
PAIR_DEV = 16
PAIRS = 512
CAP = 16
N_PAIR = 8
N_AUX = 4


def touch_ends(drawn, rng, least, top_value):
    place = [jax.random.randint(jax.random.fold_in(rng, axis), (), 0, length) for axis, length in enumerate(drawn.shape)]
    longest = drawn.shape.index(max(drawn.shape))
    next_to = place[:longest] + [(place[longest] + 1) % drawn.shape[longest]] + place[longest + 1:]
    return drawn.at[tuple(place)].set(least).at[tuple(next_to)].set(top_value)


def block_levels(own_key, dims, shards, low, largest):
    def one(position, shards_of):
        heights = jax.random.uniform(jax.random.fold_in(jax.random.fold_in(own_key, 6), position), (shards_of,), jnp.float32, low / len(shards), largest / len(shards))
        return jnp.repeat(jnp.exp(heights), dims[position] // shards_of).reshape((-1,) + (1,) * (len(dims) - position - 1))

    factor_of = one(*shards[0])
    for cut in shards[1:]:
        factor_of = factor_of * one(*cut)
    return factor_of


def different_ones(stream_key, rows, count, top, lift):
    order = jax.random.permutation(jax.random.fold_in(stream_key, 1), count)
    pull = order
    for power in range(3):
        pull = pull * pull // count
    pull = pull * lift // count
    tickets = jax.random.randint(jax.random.fold_in(stream_key, 2), (rows, count), 0, 4096) + pull
    holders = jax.random.permutation(jax.random.fold_in(stream_key, 3), rows)[jnp.arange(count) % rows]
    tickets = jnp.where(jnp.arange(rows)[:, None] == holders[None, :], 1 << 14, tickets)
    score = tickets * count + jnp.arange(count)
    return lax.top_k(score.astype(jnp.int32), top)[1].astype(jnp.int32)


def routed_block(rng, own, number, rows, number_of, top, reach, slope):
    ranking = jax.random.permutation(rng, number_of)
    heavy_load, usual = load_shares(number_of, rows * top, reach, slope, True), load_shares(number_of, rows * top, reach, slope, False)
    places = jnp.arange(number_of)

    def named(sizes, offset_by):
        used = int((sizes > 0).sum())
        fixed = max(1, used // 4)
        moved = fixed + (places - fixed + offset_by * (used - fixed)) % max(1, number_of - fixed)
        return jnp.zeros((number_of,), jnp.int32).at[ranking[jnp.where(places < fixed, places, moved)]].set(jnp.asarray(sizes, jnp.int32))

    sizes = jnp.where(number % 4 == 0, named(heavy_load, number // 4), named(usual, number - number // 4 - 1))
    mixed = jax.random.permutation(jax.random.fold_in(own, 3), number_of)
    source_of, taker = mixed[0:number_of // 2 * 2:2], mixed[1:number_of // 2 * 2:2]
    room = jnp.minimum(sizes[source_of] - 1, reach - sizes[taker]) // 2
    room = jnp.where((source_of == ranking[0]) | (taker == ranking[0]) | (sizes[taker] == 0), 0, jnp.maximum(room, 0))
    moved = jax.random.randint(jax.random.fold_in(own, 4), (number_of // 2,), 0, 1 << 20) % (room + 1)
    sizes = sizes.at[source_of].add(-moved).at[taker].add(moved)
    members = jnp.searchsorted(jnp.cumsum(sizes), jnp.arange(rows * top), side="right").astype(jnp.int32)
    listing = members.reshape(top, rows).T
    listing = listing[jax.random.permutation(jax.random.fold_in(own, 1), rows)]
    offset_by = jax.random.randint(jax.random.fold_in(own, 2), (rows, 1), 0, top)
    return jnp.take_along_axis(listing, (jnp.arange(top)[None, :] + offset_by) % top, axis=1)


def load_shares(number_of, total, bound, skew, full):
    loads = [(1 << 20) // math.isqrt(grade ** skew) + 1 for grade in range(1, number_of + 1)]
    largest = bound if full else min(bound, max(-(-total // number_of), total * loads[0] // sum(loads)))
    least = 1 if total - largest >= number_of - 1 else 0
    holding, surplus = [largest] + [least] * (number_of - 1), total - largest - least * (number_of - 1)
    while surplus > 0:
        free = [i for i in range(1, number_of) if holding[i] < largest] or [i for i in range(1, number_of) if holding[i] < bound]
        whole, left = sum([loads[i] for i in free]), surplus
        for i in free:
            addition = min(bound - holding[i], max(1, left * loads[i] // whole), surplus)
            holding[i] = holding[i] + addition
            surplus = surplus - addition
    return np.array(holding)


def scatter_about(own_key, shape, spread, most, cuts=(), kind=jnp.bfloat16):
    values = spread * jax.random.normal(own_key, shape, jnp.float32)
    if cuts:
        values = values * block_levels(own_key, shape, cuts, -0.22, 0.18)
    return jnp.clip(values, -most, most).astype(kind)


def setup_inputs(seed: int = 0) -> dict:
    streams_of = jax.random.split(jax.random.key(seed), 8)
    integrals = scatter_about(streams_of[0], (PAIRS, ADOM * ABLK, NPNO), 1.0, 6.0, ((0, 32),))
    amplitudes = scatter_about(streams_of[1], (PAIRS, NPNO, NPNO), NPNO ** -0.5, 0.75, ((0, 32),))
    pno_density = scatter_about(streams_of[2], (PAIRS, NPNO, NPNO), 1.0, 6.0, ((0, 32),))
    pno_coef = scatter_about(streams_of[3], (PAIRS, DOMB * PBLK, NPNO), NPNO ** -0.5, 0.75, ((0, 32),))
    pao_blocks = different_ones(streams_of[4], PAIRS, NBLK, DOMB, 2730)
    aux_slice_keys = jax.random.split(jax.random.fold_in(streams_of[5], 1), PAIRS // PAIR_DEV)
    aux_slice_turns = jax.random.permutation(jax.random.fold_in(streams_of[5], 3), PAIRS // PAIR_DEV)
    aux_slice = jax.vmap(lambda own, number: routed_block(jax.random.fold_in(streams_of[5], 2), own, number, PAIR_DEV, N_AUX, ADOM, CAP, 2))(aux_slice_keys, aux_slice_turns).reshape((PAIRS, ADOM))
    aux_offset = touch_ends(jax.random.randint(streams_of[6], (PAIRS, ADOM), 0, ABPO), jax.random.fold_in(streams_of[6], 1), 0, ABPO - 1).astype(jnp.int32)
    return dict(integrals=integrals, amplitudes=amplitudes, pno_density=pno_density, pno_coef=pno_coef, pao_blocks=pao_blocks, aux_slice=aux_slice, aux_offset=aux_offset)


def reference(integrals, amplitudes, pno_density, pno_coef, pao_blocks, aux_slice, aux_offset):
    block_pairs = PAIR_DEV * N_AUX
    out_scale = 1.0 / math.sqrt(PAIR_DEV * N_PAIR)

    def add_block(carry, block_index):
        gamma_acc, virt_acc = carry
        first = (block_index * block_pairs).astype(jnp.int32)

        def take(array):
            return lax.dynamic_slice_in_dim(array, first, block_pairs, 0)
        block_ints = take(integrals).astype(jnp.float32)
        block_amps = take(amplitudes).astype(jnp.float32)
        block_dens = take(pno_density).astype(jnp.float32)
        block_coef = take(pno_coef).astype(jnp.float32)
        block_pao = take(pao_blocks)
        block_rows = take(aux_slice) * ABPO + take(aux_offset)
        three_index = jnp.einsum('pqr,prs->pqs', block_ints, block_amps).astype(jnp.bfloat16)
        three_index = lax.optimization_barrier(three_index).astype(jnp.float32)
        pao_pieces = jnp.einsum('pqs,pys->pqy', three_index, block_coef).astype(jnp.bfloat16)
        pao_pieces = lax.optimization_barrier(pao_pieces).astype(jnp.float32)
        pieces = pao_pieces.reshape(block_pairs, ADOM, ABLK, DOMB, PBLK).transpose(0, 1, 3, 2, 4)
        gamma_acc = gamma_acc.at[block_rows[:, :, None], :, block_pao[:, None, :], :].add(pieces)
        weighted = jnp.einsum('pyr,prs->pys', block_coef, block_dens).astype(jnp.bfloat16)
        weighted = lax.optimization_barrier(weighted).astype(jnp.float32)
        pair_density = jnp.einsum('pys,pzs->pyz', weighted, block_coef)
        pair_density = pair_density.reshape(block_pairs, DOMB, PBLK, DOMB, PBLK).transpose(0, 1, 3, 2, 4)
        virt_acc = virt_acc.at[block_pao[:, :, None], :, block_pao[:, None, :], :].add(pair_density)
        return ((gamma_acc, virt_acc), None)
    gamma_init = jnp.zeros((N_AUX * ABPO, ABLK, NBLK, PBLK), jnp.float32)
    virt_init = jnp.zeros((NBLK, PBLK, NBLK, PBLK), jnp.float32)
    (gamma_acc, virt_acc), _ = lax.scan(add_block, (gamma_init, virt_init), jnp.arange(N_PAIR, dtype=jnp.int32))
    aux_density = gamma_acc.reshape(N_AUX * ABPO * ABLK, NBLK * PBLK) * out_scale
    virtual_density = virt_acc.reshape(NBLK * PBLK, NBLK * PBLK) * out_scale
    return (aux_density, virtual_density)
```

```python
import functools
import math

import jax
import jax.numpy as jnp
from jax import lax
from jax.experimental import pallas as pl
from jax.experimental.pallas import tpu as pltpu
from jax.sharding import PartitionSpec as P

NBLK = 6
ABPO = 4
MESH = pl.DeviceIdType.MESH
TILE = 128
SUB = 16


def by_collectives(integrals, amplitudes, pno_density, pno_coef, pao_blocks, aux_slice, aux_offset):
    n_pair = lax.axis_size("pair")
    n_aux = lax.axis_size("aux")
    pair_count, domain_rows, pno_rank = pno_coef.shape
    aux_dom = aux_slice.shape[1]
    pao_dom = pao_blocks.shape[1]
    pao_block = domain_rows // pao_dom
    aux_block = integrals.shape[1] // aux_dom
    ao_count = NBLK * pao_block
    capacity = max(2, 2 * pair_count * aux_dom // n_aux)
    out_scale = 1.0 / math.sqrt(pair_count * n_pair)
    slot_count = pair_count * aux_dom
    three_index = jnp.einsum(
        "pqr,prs->pqs", integrals, amplitudes, preferred_element_type=jnp.float32
    ).astype(jnp.bfloat16)
    owners = aux_slice.reshape(slot_count)
    owner_hot = (owners[:, None] == jnp.arange(n_aux, dtype=jnp.int32)[None, :]).astype(jnp.int32)
    before = jnp.cumsum(owner_hot, 0) - owner_hot
    slot_rank = jnp.sum(before * owner_hot, 1)
    target = owners * capacity + slot_rank
    routing = jnp.arange(n_aux * capacity, dtype=jnp.int32)[:, None] == target[None, :]
    labels = (
        jnp.concatenate(
            [aux_offset.reshape(slot_count, 1), jnp.repeat(pao_blocks, aux_dom, axis=0)], 1
        )
        + 1
    )
    label_buffer = (jnp.dot(routing.astype(jnp.int32), labels) - 1).reshape(
        n_aux, capacity, 1 + pao_dom
    )
    routing_bf = routing.astype(jnp.bfloat16)
    index_flat = three_index.reshape(slot_count, aux_block * pno_rank)
    index_buffer = jnp.dot(routing_bf, index_flat, preferred_element_type=jnp.float32).astype(
        jnp.bfloat16
    )
    index_buffer = index_buffer.reshape(n_aux, capacity, aux_block, pno_rank)
    pair_routing = (
        routing.reshape(n_aux * capacity, pair_count, aux_dom).sum(-1).astype(jnp.bfloat16)
    )
    coef_flat = pno_coef.reshape(pair_count, domain_rows * pno_rank)
    coef_buffer = jnp.dot(pair_routing, coef_flat, preferred_element_type=jnp.float32).astype(
        jnp.bfloat16
    )
    coef_buffer = coef_buffer.reshape(n_aux, capacity, domain_rows, pno_rank)
    index_part = lax.all_to_all(index_buffer, "aux", split_axis=0, concat_axis=0, tiled=True)
    coef_part = lax.all_to_all(coef_buffer, "aux", split_axis=0, concat_axis=0, tiled=True)
    label_part = lax.all_to_all(label_buffer, "aux", split_axis=0, concat_axis=0, tiled=True)
    back = jnp.einsum(
        "ncxr,ncyr->ncxy", index_part, coef_part, preferred_element_type=jnp.float32
    ).astype(jnp.bfloat16)
    got_labels = label_part
    received_count = n_aux * capacity
    pieces = back.reshape(received_count, aux_block, pao_dom, pao_block)
    got_labels = got_labels.reshape(received_count, 1 + pao_dom)
    offset_hot = got_labels[:, 0:1] == jnp.arange(ABPO, dtype=jnp.int32)[None, :]
    column_hot = got_labels[:, 1:, None] == jnp.arange(NBLK, dtype=jnp.int32)[None, None, :]
    placement = (offset_hot[:, None, :, None] & column_hot[:, :, None, :]).astype(jnp.bfloat16)
    gamma_part = jnp.einsum(
        "sxhy,shok->oxky", pieces, placement, preferred_element_type=jnp.float32
    )
    gamma_part = gamma_part.reshape(ABPO * aux_block, ao_count)
    aux_density = lax.psum_scatter(gamma_part, "pair", scatter_dimension=1, tiled=True) * out_scale
    weighted = jnp.einsum(
        "pyr,prs->pys", pno_coef, pno_density, preferred_element_type=jnp.float32
    ).astype(jnp.bfloat16)
    block_hot = (pao_blocks[:, :, None] == jnp.arange(NBLK, dtype=jnp.int32)[None, None, :]).astype(
        jnp.bfloat16
    )
    weighted_rows = jnp.einsum(
        "pak,paxr->kxpr",
        block_hot,
        weighted.reshape(pair_count, pao_dom, pao_block, pno_rank),
        preferred_element_type=jnp.float32,
    ).astype(jnp.bfloat16)
    weighted_rows = weighted_rows.reshape(ao_count, pair_count * pno_rank)
    coef_rows = jnp.einsum(
        "pak,paxr->kxpr",
        block_hot,
        pno_coef.reshape(pair_count, pao_dom, pao_block, pno_rank),
        preferred_element_type=jnp.float32,
    ).astype(jnp.bfloat16)
    coef_rows = coef_rows.reshape(ao_count, pair_count * pno_rank)
    virt_part = lax.dot_general(
        weighted_rows, coef_rows, (((1,), (1,)), ((), ())), preferred_element_type=jnp.float32
    )
    row_owned = lax.psum_scatter(virt_part, "aux", scatter_dimension=0, tiled=True)
    virtual_density = lax.psum_scatter(row_owned, "pair", scatter_dimension=1, tiled=True)
    return (aux_density, virtual_density * out_scale)


def kernel(ints, amps, dens, coef, pao, aux, off, out, coef2, tri2, wei2, ids, lhs, rhs, own, c_send, c_recv,
           ax_send, ax_recv, ay_send, ay_recv, by_send, by_recv, bx_send, bx_recv, keep1, keep2, cz_send, cz_recv,
           cw_send, cw_recv, ck, pz_send, pz_recv, pw_send, pw_recv, cx_send, cx_recv, cy_send, cy_recv, ckx,
           send_sems, recv_sems):
    pairs, rows, rank = coef.shape
    couples = pairs // 2
    width = couples * TILE
    unit = out.shape[0] // 3
    lanes = out.shape[1]
    p = lax.axis_index("pair")
    z = lax.axis_index("aux")
    c, x, y = p % 2, (p // 2) % 2, p // 4
    z0, z1 = z % 2, z // 2
    core = (p + 1 - 2 * c, z)
    xdev = (p + 2 - 4 * x, z)
    ydev = (p + 4 - 8 * y, z)
    z0dev = (p, z + 1 - 2 * z0)
    z1dev = (p, z + 2 - 4 * z1)

    barrier = pltpu.get_barrier_semaphore()
    for dev in (core, xdev, ydev, z0dev, z1dev):
        pl.semaphore_signal(barrier, inc=1, device_id=dev, device_id_type=MESH)

    started = []

    def send(src, dst, dev):
        n = len(started)
        copy = pltpu.make_async_remote_copy(
            src_ref=src, dst_ref=dst, send_sem=send_sems.at[n], recv_sem=recv_sems.at[n],
            device_id=dev, device_id_type=MESH)
        copy.start()
        started.append(copy)
        return copy

    low = lax.broadcasted_iota(jnp.int32, (SUB, TILE), 1) < rank
    for q in range(couples):
        at = slice(q * TILE, (q + 1) * TILE)
        for h in range(2):
            ids[h, :, at] = jnp.where(low, pao[2 * q, h], pao[2 * q + 1, h])
            ids[2 + h, :, at] = jnp.where(
                low,
                aux[2 * q, h] * ABPO + off[2 * q, h],
                aux[2 * q + 1, h] * ABPO + off[2 * q + 1, h])

    zero = jnp.zeros((rank, rank), jnp.bfloat16)

    def diag(ref, q):
        return jnp.concatenate(
            [jnp.concatenate([ref[2 * q], zero], 1), jnp.concatenate([zero, ref[2 * q + 1]], 1)], 0)

    def prepare(q, carry):
        at = pl.ds(pl.multiple_of(q * TILE, TILE), TILE)
        both = jnp.concatenate([coef[2 * q], coef[2 * q + 1]], 1)
        coef2[:, at] = both
        wei2[:, at] = jnp.dot(both, diag(dens, q), preferred_element_type=jnp.float32).astype(jnp.bfloat16)
        both = jnp.concatenate([ints[2 * q], ints[2 * q + 1]], 1)
        tri2[:, at] = jnp.dot(both, diag(amps, q), preferred_element_type=jnp.float32).astype(jnp.bfloat16)
        return carry

    lax.fori_loop(0, couples, prepare, 0)

    def mask(row, value):
        return jnp.where(ids[row] == value, 1.0, 0.0).astype(jnp.bfloat16)

    half_rows = rows // 2

    def place(dst, dst_row, src, src_row, count, first, value):
        m0, m1 = mask(first, value), mask(first + 1, value)
        for r in range(0, count, SUB):
            a = src[pl.ds(pl.multiple_of(src_row + r, SUB), SUB), :]
            b = src[pl.ds(pl.multiple_of(src_row + half_rows + r, SUB), SUB), :]
            dst[pl.ds(pl.multiple_of(dst_row + r, SUB), SUB), :] = a * m0 + b * m1

    per_block = half_rows // unit

    def lhs_unit(n, carry):
        half, g, i, j = n // 12, (n // 4) % 3, (n // 2) % 2, n % 2
        is_b = jnp.where(g == 1, 1, 0)
        si = is_b * j + (1 - is_b) * i
        sj = is_b * i + (1 - is_b) * j
        cc = (1 - half) * (1 - c) + half * c
        xx = (1 - si) * (1 - x) + si * x
        yy = (1 - sj) * (1 - y) + sj * y
        u = ((yy * 2 + xx) * 2 + cc) * 3 + g
        place(lhs, n * unit, coef2, (u % per_block) * unit, unit, 0, u // per_block)
        return carry

    lax.fori_loop(0, 24, lhs_unit, 0)

    chunk_of = ((1 - z1) * 2 + 1 - z0, (1 - z1) * 2 + z0, z1 * 2 + 1 - z0, z)

    def build(step):
        k = chunk_of[step]
        buf = rhs.at[step % 2]

        def aux_tile(j, carry):
            place(buf, j * TILE, tri2, 0, TILE, 2, k * ABPO + j)
            return carry

        def virt_tile(j, carry):
            place(buf, (ABPO + j) * TILE, wei2, 0, TILE, 0, 3 * (k // 2) + k % 2 + j)
            return carry

        lax.fori_loop(0, ABPO, aux_tile, 0)
        lax.fori_loop(0, 2, virt_tile, 0)

    n_rows = 12 * unit
    wide = 2 * TILE

    def product(step, half, dst, kind):
        left = lhs.at[pl.ds(half * n_rows, n_rows)]

        def body(t, carry):
            at = pl.ds(pl.multiple_of(t * wide, wide), wide)
            dst[:, at] = lax.dot_general(
                left[...], rhs[step % 2, at, :], (((1,), (1,)), ((), ())),
                preferred_element_type=jnp.float32).astype(kind)
            return carry

        lax.fori_loop(0, lanes // wide, body, 0)

    f32, bf16 = jnp.float32, jnp.bfloat16
    u2, u4 = 2 * unit, 4 * unit
    stage1 = {}
    stage2 = {}
    zcopy = {}

    def first(step):
        stage1[step, "c"].wait_recv()

        def summed(lo, hi):
            return own[lo:hi, :] + c_recv[step, lo:hi, :].astype(f32)

        ax_send[step] = summed(0, u2).astype(bf16)
        stage1[step, "a"] = send(ax_send.at[step], ax_recv.at[step], xdev)
        by_send[step] = summed(u4, u4 + u2).astype(bf16)
        stage1[step, "b"] = send(by_send.at[step], by_recv.at[step], ydev)
        if step in (0, 2):
            cz_send[step // 2] = summed(2 * u4, 3 * u4).astype(bf16)
            zcopy["c", step] = send(cz_send.at[step // 2], cz_recv.at[step // 2], z0dev)
        else:
            ck[step // 2] = summed(2 * u4, 3 * u4)
        keep1[step, 0:u2] = summed(u2, u4)
        keep1[step, u2:u4] = summed(u4 + u2, 2 * u4)

    def second(step):
        stage1[step, "a"].wait_recv()
        ay_send[step] = (keep1[step, 0:unit] + ax_recv[step, 0:unit].astype(f32)).astype(bf16)
        stage2[step, "a"] = send(ay_send.at[step], ay_recv.at[step], ydev)
        keep2[step, 0:unit] = keep1[step, unit:u2] + ax_recv[step, unit:u2].astype(f32)
        stage1[step, "b"].wait_recv()
        bx_send[step] = (keep1[step, u2:u2 + unit] + by_recv[step, 0:unit].astype(f32)).astype(bf16)
        stage2[step, "b"] = send(bx_send.at[step], bx_recv.at[step], xdev)
        keep2[step, unit:u2] = keep1[step, u2 + unit:u4] + by_recv[step, unit:u2].astype(f32)

    def third_sum(step, lo, hi):
        got = ay_recv if lo == 0 else bx_recv
        return keep2[step, lo:hi] + got[step].astype(f32)

    def third(step):
        stage2[step, "a"].wait_recv()
        stage2[step, "b"].wait_recv()
        halves = ((0, unit), (unit, u2))
        if step in (0, 2):
            for lo, hi in halves:
                pz_send[step // 2, lo:hi] = third_sum(step, lo, hi).astype(bf16)
            zcopy["p", step] = send(pz_send.at[step // 2], pz_recv.at[step // 2], z0dev)
        elif step == 1:
            zcopy["p", 0].wait_recv()
            for lo, hi in halves:
                pw_send[lo:hi] = (third_sum(step, lo, hi) + pz_recv[0, lo:hi].astype(f32)).astype(bf16)
            zcopy["p", 1] = send(pw_send, pw_recv, z1dev)
        else:
            zcopy["p", 2].wait_recv()
            zcopy["p", 1].wait_recv()
            for lo, hi in halves:
                out[lo:hi] = third_sum(step, lo, hi) + pz_recv[1, lo:hi].astype(f32) + pw_recv[lo:hi].astype(f32)

    def c_across():
        zcopy["c", 0].wait_recv()
        cw_send[...] = (ck[0] + cz_recv[0].astype(f32)).astype(bf16)
        zcopy["c", 1] = send(cw_send, cw_recv, z1dev)

    build(0)
    for step in range(4):
        product(step, 0, c_send.at[step], bf16)
        if step == 0:
            pl.semaphore_wait(barrier, 5)
        stage1[step, "c"] = send(c_send.at[step], c_recv.at[step], core)
        product(step, 1, own, f32)
        if step < 3:
            build(step + 1)
        first(step)
        if step >= 1:
            second(step - 1)
        if step == 1:
            c_across()
        if step >= 2:
            third(step - 2)

    second(3)
    third(2)
    zcopy["c", 2].wait_recv()
    zcopy["c", 1].wait_recv()

    def c_sum(lo, hi):
        return ck[1, lo:hi] + cz_recv[1, lo:hi].astype(f32) + cw_recv[lo:hi].astype(f32)

    cx_send[...] = c_sum(0, u2).astype(bf16)
    cx = send(cx_send, cx_recv, xdev)
    ckx[...] = c_sum(u2, u4)
    third(3)
    cx.wait_recv()
    cy_send[...] = (ckx[0:unit] + cx_recv[0:unit].astype(f32)).astype(bf16)
    cy = send(cy_send, cy_recv, ydev)
    ckx[unit:u2] = ckx[unit:u2] + cx_recv[unit:u2].astype(f32)
    cy.wait_recv()
    out[u2:3 * unit] = ckx[unit:u2] + cy_recv[...].astype(f32)
    for copy in started:
        copy.wait_send()


COPIES = 4 + 8 + 8 + 2 + 1 + 2 + 1 + 2


def by_kernel(integrals, amplitudes, pno_density, pno_coef, pao_blocks, aux_slice, aux_offset):
    n_pair = lax.axis_size("pair")
    n_aux = lax.axis_size("aux")
    pairs, rows, rank = pno_coef.shape
    block = rows // pao_blocks.shape[1]
    ao_count = NBLK * block
    shard = ao_count // n_pair
    unit = shard // 3
    aux_lanes = ABPO * block
    lanes = aux_lanes + 2 * block
    width = pairs * rank
    scale = 1.0 / math.sqrt(pairs * n_pair)
    vmem = pl.BlockSpec(memory_space=pltpu.VMEM)
    smem = pl.BlockSpec(memory_space=pltpu.SMEM)

    def half(*dims):
        return pltpu.VMEM(dims + (lanes,), jnp.bfloat16)

    def full(*dims):
        return pltpu.VMEM(dims + (lanes,), jnp.float32)

    u1, u2, u4 = unit, 2 * unit, 4 * unit
    out = pl.pallas_call(
        kernel,
        out_shape=jax.ShapeDtypeStruct((shard, lanes), jnp.float32),
        in_specs=[vmem] * 4 + [smem] * 3,
        out_specs=vmem,
        scratch_shapes=[
            pltpu.VMEM((rows, width), jnp.bfloat16),
            pltpu.VMEM((rows, width), jnp.bfloat16),
            pltpu.VMEM((rows, width), jnp.bfloat16),
            pltpu.VMEM((4, SUB, width), jnp.int32),
            pltpu.VMEM((24 * unit, width), jnp.bfloat16),
            pltpu.VMEM((2, lanes, width), jnp.bfloat16),
            full(12 * unit),
            half(4, 12 * unit), half(4, 12 * unit),
            half(4, u2), half(4, u2), half(4, u1), half(4, u1),
            half(4, u2), half(4, u2), half(4, u1), half(4, u1),
            full(4, u4), full(4, u2),
            half(2, u4), half(2, u4), half(u4), half(u4), full(2, u4),
            half(2, u2), half(2, u2), half(u2), half(u2),
            half(u2), half(u2), half(u1), half(u1), full(u2),
            pltpu.SemaphoreType.DMA((COPIES,)),
            pltpu.SemaphoreType.DMA((COPIES,)),
        ],
        compiler_params=pltpu.CompilerParams(
            collective_id=0, has_side_effects=True, vmem_limit_bytes=60 * 1024 * 1024),
    )(integrals, amplitudes, pno_density, pno_coef, pao_blocks, aux_slice, aux_offset)
    strip = ao_count // n_aux
    start = (lax.axis_index("aux") % 2) * (2 * block - strip)
    virt = lax.dynamic_slice(out, (0, aux_lanes + start), (shard, strip))
    return out[:, :aux_lanes].T * scale, virt.T * scale


def on_device(*args):
    pairs, rows, rank = args[3].shape
    fits = lax.axis_size("pair") == 8 and lax.axis_size("aux") == 4 and pairs % 2 == 0 and 2 * rank == TILE
    fits = fits and rows == 2 * TILE and args[0].shape[1] == 2 * TILE
    return by_kernel(*args) if fits else by_collectives(*args)


def solution(mesh):
    in_specs = (
        P(("pair", "aux"), None, None),
        P(("pair", "aux"), None, None),
        P(("pair", "aux"), None, None),
        P(("pair", "aux"), None, None),
        P(("pair", "aux"), None),
        P(("pair", "aux"), None),
        P(("pair", "aux"), None),
    )
    out_specs = (P("aux", "pair"), P("aux", "pair"))
    return jax.shard_map(
        on_device, mesh=mesh, in_specs=in_specs, out_specs=out_specs, check_vma=False
    )
```

```python
import functools
import math

import jax
import jax.numpy as jnp
from jax import lax
from jax.experimental import pallas as pl
from jax.experimental.pallas import tpu as pltpu
from jax.sharding import PartitionSpec as P

NBLK = 6
ABPO = 4
MESH = pl.DeviceIdType.MESH
TILE = 128
SUB = 16


def by_collectives(integrals, amplitudes, pno_density, pno_coef, pao_blocks, aux_slice, aux_offset):
    n_pair = lax.axis_size("pair")
    n_aux = lax.axis_size("aux")
    pair_count, domain_rows, pno_rank = pno_coef.shape
    aux_dom = aux_slice.shape[1]
    pao_dom = pao_blocks.shape[1]
    pao_block = domain_rows // pao_dom
    aux_block = integrals.shape[1] // aux_dom
    ao_count = NBLK * pao_block
    capacity = max(2, 2 * pair_count * aux_dom // n_aux)
    out_scale = 1.0 / math.sqrt(pair_count * n_pair)
    slot_count = pair_count * aux_dom
    three_index = jnp.einsum(
        "pqr,prs->pqs", integrals, amplitudes, preferred_element_type=jnp.float32
    ).astype(jnp.bfloat16)
    owners = aux_slice.reshape(slot_count)
    owner_hot = (owners[:, None] == jnp.arange(n_aux, dtype=jnp.int32)[None, :]).astype(jnp.int32)
    before = jnp.cumsum(owner_hot, 0) - owner_hot
    slot_rank = jnp.sum(before * owner_hot, 1)
    target = owners * capacity + slot_rank
    routing = jnp.arange(n_aux * capacity, dtype=jnp.int32)[:, None] == target[None, :]
    labels = (
        jnp.concatenate(
            [aux_offset.reshape(slot_count, 1), jnp.repeat(pao_blocks, aux_dom, axis=0)], 1
        )
        + 1
    )
    label_buffer = (jnp.dot(routing.astype(jnp.int32), labels) - 1).reshape(
        n_aux, capacity, 1 + pao_dom
    )
    routing_bf = routing.astype(jnp.bfloat16)
    index_flat = three_index.reshape(slot_count, aux_block * pno_rank)
    index_buffer = jnp.dot(routing_bf, index_flat, preferred_element_type=jnp.float32).astype(
        jnp.bfloat16
    )
    index_buffer = index_buffer.reshape(n_aux, capacity, aux_block, pno_rank)
    pair_routing = (
        routing.reshape(n_aux * capacity, pair_count, aux_dom).sum(-1).astype(jnp.bfloat16)
    )
    coef_flat = pno_coef.reshape(pair_count, domain_rows * pno_rank)
    coef_buffer = jnp.dot(pair_routing, coef_flat, preferred_element_type=jnp.float32).astype(
        jnp.bfloat16
    )
    coef_buffer = coef_buffer.reshape(n_aux, capacity, domain_rows, pno_rank)
    index_part = lax.all_to_all(index_buffer, "aux", split_axis=0, concat_axis=0, tiled=True)
    coef_part = lax.all_to_all(coef_buffer, "aux", split_axis=0, concat_axis=0, tiled=True)
    label_part = lax.all_to_all(label_buffer, "aux", split_axis=0, concat_axis=0, tiled=True)
    back = jnp.einsum(
        "ncxr,ncyr->ncxy", index_part, coef_part, preferred_element_type=jnp.float32
    ).astype(jnp.bfloat16)
    got_labels = label_part
    received_count = n_aux * capacity
    pieces = back.reshape(received_count, aux_block, pao_dom, pao_block)
    got_labels = got_labels.reshape(received_count, 1 + pao_dom)
    offset_hot = got_labels[:, 0:1] == jnp.arange(ABPO, dtype=jnp.int32)[None, :]
    column_hot = got_labels[:, 1:, None] == jnp.arange(NBLK, dtype=jnp.int32)[None, None, :]
    placement = (offset_hot[:, None, :, None] & column_hot[:, :, None, :]).astype(jnp.bfloat16)
    gamma_part = jnp.einsum(
        "sxhy,shok->oxky", pieces, placement, preferred_element_type=jnp.float32
    )
    gamma_part = gamma_part.reshape(ABPO * aux_block, ao_count)
    aux_density = lax.psum_scatter(gamma_part, "pair", scatter_dimension=1, tiled=True) * out_scale
    weighted = jnp.einsum(
        "pyr,prs->pys", pno_coef, pno_density, preferred_element_type=jnp.float32
    ).astype(jnp.bfloat16)
    block_hot = (pao_blocks[:, :, None] == jnp.arange(NBLK, dtype=jnp.int32)[None, None, :]).astype(
        jnp.bfloat16
    )
    weighted_rows = jnp.einsum(
        "pak,paxr->kxpr",
        block_hot,
        weighted.reshape(pair_count, pao_dom, pao_block, pno_rank),
        preferred_element_type=jnp.float32,
    ).astype(jnp.bfloat16)
    weighted_rows = weighted_rows.reshape(ao_count, pair_count * pno_rank)
    coef_rows = jnp.einsum(
        "pak,paxr->kxpr",
        block_hot,
        pno_coef.reshape(pair_count, pao_dom, pao_block, pno_rank),
        preferred_element_type=jnp.float32,
    ).astype(jnp.bfloat16)
    coef_rows = coef_rows.reshape(ao_count, pair_count * pno_rank)
    virt_part = lax.dot_general(
        weighted_rows, coef_rows, (((1,), (1,)), ((), ())), preferred_element_type=jnp.float32
    )
    row_owned = lax.psum_scatter(virt_part, "aux", scatter_dimension=0, tiled=True)
    virtual_density = lax.psum_scatter(row_owned, "pair", scatter_dimension=1, tiled=True)
    return (aux_density, virtual_density * out_scale)


def kernel(scale, ints, amps, dens, coef, pao, aux, off, gamma, virt, out, coef2, tri2, wei2, ids, lhs, rhs, own, c_send, c_recv,
           ax_send, ax_recv, ay_send, ay_recv, by_send, by_recv, bx_send, bx_recv, keep1, keep2, cz_send, cz_recv,
           cw_send, cw_recv, ck, pz_send, pz_recv, pw_send, pw_recv, cx_send, cx_recv, cy_send, cy_recv, ckx, turned,
           send_sems, recv_sems):
    pairs, rank, rows = coef.shape
    couples = pairs // 2
    unit = gamma.shape[0] // 3
    lanes = out.shape[1]
    p = lax.axis_index("pair")
    z = lax.axis_index("aux")
    c, x, y = p % 2, (p // 2) % 2, p // 4
    z0, z1 = z % 2, z // 2
    core = (p + 1 - 2 * c, z)
    xdev = (p + 2 - 4 * x, z)
    ydev = (p + 4 - 8 * y, z)
    z0dev = (p, z + 1 - 2 * z0)
    z1dev = (p, z + 2 - 4 * z1)

    barrier = pltpu.get_barrier_semaphore()
    for dev in (core, xdev, ydev, z0dev, z1dev):
        pl.semaphore_signal(barrier, inc=1, device_id=dev, device_id_type=MESH)

    started = []

    def send(src, dst, dev):
        n = len(started)
        copy = pltpu.make_async_remote_copy(
            src_ref=src, dst_ref=dst, send_sem=send_sems.at[n], recv_sem=recv_sems.at[n],
            device_id=dev, device_id_type=MESH)
        copy.start()
        started.append(copy)
        return copy

    low = lax.broadcasted_iota(jnp.int32, (SUB, TILE), 1) < rank
    for q in range(couples):
        at = slice(q * TILE, (q + 1) * TILE)
        for h in range(2):
            ids[h, :, at] = jnp.where(low, pao[h, 2 * q], pao[h, 2 * q + 1])

    zero = jnp.zeros((rank, rank), jnp.bfloat16)

    def mixed(ref, q, both):
        diag = jnp.concatenate(
            [jnp.concatenate([ref[2 * q], zero], 1), jnp.concatenate([zero, ref[2 * q + 1]], 1)], 0)
        return lax.dot_general(
            diag, both, (((0,), (0,)), ((), ())), preferred_element_type=jnp.float32).astype(jnp.bfloat16)

    for q in range(couples):
        at = slice(q * TILE, (q + 1) * TILE)
        both = coef[2 * q:2 * q + 2].reshape(2 * rank, rows)
        coef2[:, at] = both.T
        wei2[at, :] = mixed(dens, q, both)
        tri2[at, :] = mixed(amps, q, ints[2 * q:2 * q + 2].reshape(2 * rank, rows))

    def mask(row, value):
        return jnp.where(ids[row] == value, 1.0, 0.0).astype(jnp.bfloat16)

    half_rows = rows // 2

    def place(dst, dst_row, src, src_row, count, first, value):
        m0, m1 = mask(first, value), mask(first + 1, value)
        for r in range(0, count, SUB):
            a = src[pl.ds(pl.multiple_of(src_row + r, SUB), SUB), :]
            b = src[pl.ds(pl.multiple_of(src_row + half_rows + r, SUB), SUB), :]
            dst[pl.ds(pl.multiple_of(dst_row + r, SUB), SUB), :] = a * m0 + b * m1

    per_block = half_rows // unit

    def lhs_unit(n, carry):
        half, g, i, j = n // 12, (n // 4) % 3, (n // 2) % 2, n % 2
        is_b = jnp.where(g == 1, 1, 0)
        si = is_b * j + (1 - is_b) * i
        sj = is_b * i + (1 - is_b) * j
        cc = (1 - half) * (1 - c) + half * c
        xx = (1 - si) * (1 - x) + si * x
        yy = (1 - sj) * (1 - y) + sj * y
        u = ((yy * 2 + xx) * 2 + cc) * 3 + g
        place(lhs, n * unit, coef2, (u % per_block) * unit, unit, 0, u // per_block)
        return carry

    lax.fori_loop(0, 24, lhs_unit, 0)

    chunk_of = ((1 - z1) * 2 + 1 - z0, (1 - z1) * 2 + z0, z1 * 2 + 1 - z0, z)

    def build(step):
        k = chunk_of[step]
        virt_first = 3 * (k // 2) + k % 2

        def switch(label, value):
            return jnp.full((rank, TILE), jnp.where(label == value, 1.0, 0.0), jnp.float32).astype(jnp.bfloat16)

        def one_pair(n, carry):
            at = pl.ds(pl.multiple_of(n * rank, rank), rank)
            for src, blocks, labels, start, base in (
                (tri2, ABPO, [aux[h, n] * ABPO + off[h, n] for h in range(2)], k * ABPO, 0),
                (wei2, 2, [pao[h, n] for h in range(2)], virt_first, ABPO),
            ):
                low_part, high_part = src[at, 0:TILE], src[at, TILE:2 * TILE]
                for j in range(blocks):
                    rhs[step % 2, at, (base + j) * TILE:(base + j + 1) * TILE] = (
                        low_part * switch(labels[0], start + j) + high_part * switch(labels[1], start + j))
            return carry

        lax.fori_loop(0, pairs, one_pair, 0, unroll=2)

    n_rows = 12 * unit
    wide = 2 * TILE

    def product(step, half, dst, kind):
        left = lhs.at[pl.ds(half * n_rows, n_rows)]

        def body(t, carry):
            at = pl.ds(pl.multiple_of(t * wide, wide), wide)
            dst[:, at] = lax.dot_general(
                left[...], rhs[step % 2, :, at], (((1,), (0,)), ((), ())),
                preferred_element_type=jnp.float32).astype(kind)
            return carry

        lax.fori_loop(0, lanes // wide, body, 0)

    f32, bf16 = jnp.float32, jnp.bfloat16
    u2, u4 = 2 * unit, 4 * unit
    stage1 = {}
    stage2 = {}
    zcopy = {}

    def first(step):
        stage1[step, "c"].wait_recv()

        def summed(lo, hi):
            return own[lo:hi, :] + c_recv[step, lo:hi, :].astype(f32)

        ax_send[step] = summed(0, u2).astype(bf16)
        stage1[step, "a"] = send(ax_send.at[step], ax_recv.at[step], xdev)
        by_send[step] = summed(u4, u4 + u2).astype(bf16)
        stage1[step, "b"] = send(by_send.at[step], by_recv.at[step], ydev)
        if step in (0, 2):
            cz_send[step // 2] = summed(2 * u4, 3 * u4).astype(bf16)
            zcopy["c", step] = send(cz_send.at[step // 2], cz_recv.at[step // 2], z0dev)
        else:
            ck[step // 2] = summed(2 * u4, 3 * u4)
        keep1[step, 0:u2] = summed(u2, u4)
        keep1[step, u2:u4] = summed(u4 + u2, 2 * u4)

    def second(step):
        stage1[step, "a"].wait_recv()
        ay_send[step] = (keep1[step, 0:unit] + ax_recv[step, 0:unit].astype(f32)).astype(bf16)
        stage2[step, "a"] = send(ay_send.at[step], ay_recv.at[step], ydev)
        keep2[step, 0:unit] = keep1[step, unit:u2] + ax_recv[step, unit:u2].astype(f32)
        stage1[step, "b"].wait_recv()
        bx_send[step] = (keep1[step, u2:u2 + unit] + by_recv[step, 0:unit].astype(f32)).astype(bf16)
        stage2[step, "b"] = send(bx_send.at[step], bx_recv.at[step], xdev)
        keep2[step, unit:u2] = keep1[step, u2 + unit:u4] + by_recv[step, unit:u2].astype(f32)

    def third_sum(step, lo, hi):
        got = ay_recv if lo == 0 else bx_recv
        return keep2[step, lo:hi] + got[step].astype(f32)

    def third(step):
        stage2[step, "a"].wait_recv()
        stage2[step, "b"].wait_recv()
        halves = ((0, unit), (unit, u2))
        if step in (0, 2):
            for lo, hi in halves:
                pz_send[step // 2, lo:hi] = third_sum(step, lo, hi).astype(bf16)
            zcopy["p", step] = send(pz_send.at[step // 2], pz_recv.at[step // 2], z0dev)
        elif step == 1:
            zcopy["p", 0].wait_recv()
            for lo, hi in halves:
                pw_send[lo:hi] = (third_sum(step, lo, hi) + pz_recv[0, lo:hi].astype(f32)).astype(bf16)
            zcopy["p", 1] = send(pw_send, pw_recv, z1dev)
        else:
            zcopy["p", 2].wait_recv()
            zcopy["p", 1].wait_recv()
            for lo, hi in halves:
                out[lo:hi] = third_sum(step, lo, hi) + pz_recv[1, lo:hi].astype(f32) + pw_recv[lo:hi].astype(f32)

    def c_across():
        zcopy["c", 0].wait_recv()
        cw_send[...] = (ck[0] + cz_recv[0].astype(f32)).astype(bf16)
        zcopy["c", 1] = send(cw_send, cw_recv, z1dev)

    build(0)
    for step in range(4):
        product(step, 0, c_send.at[step], bf16)
        if step == 0:
            pl.semaphore_wait(barrier, 5)
        stage1[step, "c"] = send(c_send.at[step], c_recv.at[step], core)
        product(step, 1, own, f32)
        if step < 3:
            build(step + 1)
        first(step)
        if step >= 1:
            second(step - 1)
        if step == 1:
            c_across()
        if step >= 2:
            third(step - 2)

    second(3)
    third(2)
    zcopy["c", 2].wait_recv()
    zcopy["c", 1].wait_recv()

    def c_sum(lo, hi):
        return ck[1, lo:hi] + cz_recv[1, lo:hi].astype(f32) + cw_recv[lo:hi].astype(f32)

    cx_send[...] = c_sum(0, u2).astype(bf16)
    cx = send(cx_send, cx_recv, xdev)
    ckx[...] = c_sum(u2, u4)
    third(3)
    cx.wait_recv()
    cy_send[...] = (ckx[0:unit] + cx_recv[0:unit].astype(f32)).astype(bf16)
    cy = send(cy_send, cy_recv, ydev)
    ckx[unit:u2] = ckx[unit:u2] + cx_recv[unit:u2].astype(f32)
    cy.wait_recv()
    out[u2:3 * unit] = ckx[unit:u2] + cy_recv[...].astype(f32)
    aux_lanes = gamma.shape[1]
    gamma[...] = out[0:3 * unit, 0:aux_lanes] * scale
    out[3 * unit:] = jnp.zeros((out.shape[0] - 3 * unit, lanes), f32)
    turned[...] = out[:, aux_lanes:].T * scale
    strip = virt.shape[0]
    virt[...] = turned[pl.ds(pl.multiple_of(z0 * (turned.shape[0] - strip), 8), strip), 0:3 * unit]
    for copy in started:
        copy.wait_send()


COPIES = 4 + 8 + 8 + 2 + 1 + 2 + 1 + 2


def by_kernel(integrals, amplitudes, pno_density, pno_coef, pao_blocks, aux_slice, aux_offset):
    n_pair = lax.axis_size("pair")
    n_aux = lax.axis_size("aux")
    pairs, rows, rank = pno_coef.shape
    block = rows // pao_blocks.shape[1]
    ao_count = NBLK * block
    shard = ao_count // n_pair
    unit = shard // 3
    aux_lanes = ABPO * block
    lanes = aux_lanes + 2 * block
    width = pairs * rank
    scale = 1.0 / math.sqrt(pairs * n_pair)
    vmem = pl.BlockSpec(memory_space=pltpu.VMEM)
    smem = pl.BlockSpec(memory_space=pltpu.SMEM)

    def half(*dims):
        return pltpu.VMEM(dims + (lanes,), jnp.bfloat16)

    def full(*dims):
        return pltpu.VMEM(dims + (lanes,), jnp.float32)

    u1, u2, u4 = unit, 2 * unit, 4 * unit
    gamma, virt = pl.pallas_call(
        functools.partial(kernel, scale),
        out_shape=[
            jax.ShapeDtypeStruct((shard, aux_lanes), jnp.float32),
            jax.ShapeDtypeStruct((ao_count // n_aux, shard), jnp.float32),
        ],
        in_specs=[vmem] * 4 + [smem] * 3,
        out_specs=[vmem] * 2,
        scratch_shapes=[
            full(TILE),
            pltpu.VMEM((rows, width), jnp.bfloat16),
            pltpu.VMEM((width, rows), jnp.bfloat16),
            pltpu.VMEM((width, rows), jnp.bfloat16),
            pltpu.VMEM((2, SUB, width), jnp.int32),
            pltpu.VMEM((24 * unit, width), jnp.bfloat16),
            pltpu.VMEM((2, width, lanes), jnp.bfloat16),
            full(12 * unit),
            half(4, 12 * unit), half(4, 12 * unit),
            half(4, u2), half(4, u2), half(4, u1), half(4, u1),
            half(4, u2), half(4, u2), half(4, u1), half(4, u1),
            full(4, u4), full(4, u2),
            half(2, u4), half(2, u4), half(u4), half(u4), full(2, u4),
            half(2, u2), half(2, u2), half(u2), half(u2),
            half(u2), half(u2), half(u1), half(u1), full(u2),
            pltpu.VMEM((2 * block, TILE), jnp.float32),
            pltpu.SemaphoreType.DMA((COPIES,)),
            pltpu.SemaphoreType.DMA((COPIES,)),
        ],
        compiler_params=pltpu.CompilerParams(
            collective_id=0, has_side_effects=True, vmem_limit_bytes=60 * 1024 * 1024),
    )(integrals.swapaxes(1, 2), amplitudes, pno_density, pno_coef.swapaxes(1, 2),
      pao_blocks.T, aux_slice.T, aux_offset.T)
    return gamma.T, virt


def on_device(*args):
    pairs, rows, rank = args[3].shape
    fits = lax.axis_size("pair") == 8 and lax.axis_size("aux") == 4 and pairs % 2 == 0 and 2 * rank == TILE
    fits = fits and rows == 2 * TILE and args[0].shape[1] == 2 * TILE
    return by_kernel(*args) if fits else by_collectives(*args)


def solution(mesh):
    in_specs = (
        P(("pair", "aux"), None, None),
        P(("pair", "aux"), None, None),
        P(("pair", "aux"), None, None),
        P(("pair", "aux"), None, None),
        P(("pair", "aux"), None),
        P(("pair", "aux"), None),
        P(("pair", "aux"), None),
    )
    out_specs = (P("aux", "pair"), P("aux", "pair"))
    return jax.shard_map(
        on_device, mesh=mesh, in_specs=in_specs, out_specs=out_specs, check_vma=False
    )
```

```python
import functools
import math

import jax
import jax.numpy as jnp
from jax import lax
from jax.experimental import pallas as pl
from jax.experimental.pallas import tpu as pltpu
from jax.sharding import PartitionSpec as P

NBLK = 6
ABPO = 4
MESH = pl.DeviceIdType.MESH
TILE = 128
SUB = 16


def by_collectives(integrals, amplitudes, pno_density, pno_coef, pao_blocks, aux_slice, aux_offset):
    n_pair = lax.axis_size("pair")
    n_aux = lax.axis_size("aux")
    pair_count, domain_rows, pno_rank = pno_coef.shape
    aux_dom = aux_slice.shape[1]
    pao_dom = pao_blocks.shape[1]
    pao_block = domain_rows // pao_dom
    aux_block = integrals.shape[1] // aux_dom
    ao_count = NBLK * pao_block
    capacity = max(2, 2 * pair_count * aux_dom // n_aux)
    out_scale = 1.0 / math.sqrt(pair_count * n_pair)
    slot_count = pair_count * aux_dom
    three_index = jnp.einsum(
        "pqr,prs->pqs", integrals, amplitudes, preferred_element_type=jnp.float32
    ).astype(jnp.bfloat16)
    owners = aux_slice.reshape(slot_count)
    owner_hot = (owners[:, None] == jnp.arange(n_aux, dtype=jnp.int32)[None, :]).astype(jnp.int32)
    before = jnp.cumsum(owner_hot, 0) - owner_hot
    slot_rank = jnp.sum(before * owner_hot, 1)
    target = owners * capacity + slot_rank
    routing = jnp.arange(n_aux * capacity, dtype=jnp.int32)[:, None] == target[None, :]
    labels = (
        jnp.concatenate(
            [aux_offset.reshape(slot_count, 1), jnp.repeat(pao_blocks, aux_dom, axis=0)], 1
        )
        + 1
    )
    label_buffer = (jnp.dot(routing.astype(jnp.int32), labels) - 1).reshape(
        n_aux, capacity, 1 + pao_dom
    )
    routing_bf = routing.astype(jnp.bfloat16)
    index_flat = three_index.reshape(slot_count, aux_block * pno_rank)
    index_buffer = jnp.dot(routing_bf, index_flat, preferred_element_type=jnp.float32).astype(
        jnp.bfloat16
    )
    index_buffer = index_buffer.reshape(n_aux, capacity, aux_block, pno_rank)
    pair_routing = (
        routing.reshape(n_aux * capacity, pair_count, aux_dom).sum(-1).astype(jnp.bfloat16)
    )
    coef_flat = pno_coef.reshape(pair_count, domain_rows * pno_rank)
    coef_buffer = jnp.dot(pair_routing, coef_flat, preferred_element_type=jnp.float32).astype(
        jnp.bfloat16
    )
    coef_buffer = coef_buffer.reshape(n_aux, capacity, domain_rows, pno_rank)
    index_part = lax.all_to_all(index_buffer, "aux", split_axis=0, concat_axis=0, tiled=True)
    coef_part = lax.all_to_all(coef_buffer, "aux", split_axis=0, concat_axis=0, tiled=True)
    label_part = lax.all_to_all(label_buffer, "aux", split_axis=0, concat_axis=0, tiled=True)
    back = jnp.einsum(
        "ncxr,ncyr->ncxy", index_part, coef_part, preferred_element_type=jnp.float32
    ).astype(jnp.bfloat16)
    got_labels = label_part
    received_count = n_aux * capacity
    pieces = back.reshape(received_count, aux_block, pao_dom, pao_block)
    got_labels = got_labels.reshape(received_count, 1 + pao_dom)
    offset_hot = got_labels[:, 0:1] == jnp.arange(ABPO, dtype=jnp.int32)[None, :]
    column_hot = got_labels[:, 1:, None] == jnp.arange(NBLK, dtype=jnp.int32)[None, None, :]
    placement = (offset_hot[:, None, :, None] & column_hot[:, :, None, :]).astype(jnp.bfloat16)
    gamma_part = jnp.einsum(
        "sxhy,shok->oxky", pieces, placement, preferred_element_type=jnp.float32
    )
    gamma_part = gamma_part.reshape(ABPO * aux_block, ao_count)
    aux_density = lax.psum_scatter(gamma_part, "pair", scatter_dimension=1, tiled=True) * out_scale
    weighted = jnp.einsum(
        "pyr,prs->pys", pno_coef, pno_density, preferred_element_type=jnp.float32
    ).astype(jnp.bfloat16)
    block_hot = (pao_blocks[:, :, None] == jnp.arange(NBLK, dtype=jnp.int32)[None, None, :]).astype(
        jnp.bfloat16
    )
    weighted_rows = jnp.einsum(
        "pak,paxr->kxpr",
        block_hot,
        weighted.reshape(pair_count, pao_dom, pao_block, pno_rank),
        preferred_element_type=jnp.float32,
    ).astype(jnp.bfloat16)
    weighted_rows = weighted_rows.reshape(ao_count, pair_count * pno_rank)
    coef_rows = jnp.einsum(
        "pak,paxr->kxpr",
        block_hot,
        pno_coef.reshape(pair_count, pao_dom, pao_block, pno_rank),
        preferred_element_type=jnp.float32,
    ).astype(jnp.bfloat16)
    coef_rows = coef_rows.reshape(ao_count, pair_count * pno_rank)
    virt_part = lax.dot_general(
        weighted_rows, coef_rows, (((1,), (1,)), ((), ())), preferred_element_type=jnp.float32
    )
    row_owned = lax.psum_scatter(virt_part, "aux", scatter_dimension=0, tiled=True)
    virtual_density = lax.psum_scatter(row_owned, "pair", scatter_dimension=1, tiled=True)
    return (aux_density, virtual_density * out_scale)


def group_rows(shard):
    units = shard // SUB
    c = max(1, units // 6)
    a = units // 2
    return a * SUB, (units - a - c) * SUB, c * SUB


def kernel(scale, ints, amps, dens, coef, pao, aux, off, gamma, virt, out, coef2, tri2, wei2, ids, lhs, rhs, own, c_send, c_recv,
           ax_send, ax_recv, ay_send, ay_recv, by_send, by_recv, bx_send, bx_recv, keep1, keep2, cz_send, cz_recv,
           cw_send, cw_recv, ck, pz_send, pz_recv, pw_send, pw_recv, cx_send, cx_recv, cy_send, cy_recv, ckx, turned,
           send_sems, recv_sems):
    pairs, rank, rows = coef.shape
    couples = pairs // 2
    shard = gamma.shape[0]
    na, nb, nc = group_rows(shard)
    nab = na + nb
    lanes = out.shape[1]
    p = lax.axis_index("pair")
    z = lax.axis_index("aux")
    c, x, y = p % 2, (p // 2) % 2, p // 4
    z0, z1 = z % 2, z // 2
    core = (p + 1 - 2 * c, z)
    xdev = (p + 2 - 4 * x, z)
    ydev = (p + 4 - 8 * y, z)
    z0dev = (p, z + 1 - 2 * z0)
    z1dev = (p, z + 2 - 4 * z1)

    barrier = pltpu.get_barrier_semaphore()
    for dev in (core, xdev, ydev, z0dev, z1dev):
        pl.semaphore_signal(barrier, inc=1, device_id=dev, device_id_type=MESH)

    started = []

    def send(src, dst, dev):
        n = len(started)
        copy = pltpu.make_async_remote_copy(
            src_ref=src, dst_ref=dst, send_sem=send_sems.at[n], recv_sem=recv_sems.at[n],
            device_id=dev, device_id_type=MESH)
        copy.start()
        started.append(copy)
        return copy

    low = lax.broadcasted_iota(jnp.int32, (SUB, TILE), 1) < rank
    for q in range(couples):
        at = slice(q * TILE, (q + 1) * TILE)
        for h in range(2):
            ids[h, :, at] = jnp.where(low, pao[h, 2 * q], pao[h, 2 * q + 1])

    zero = jnp.zeros((rank, rank), jnp.bfloat16)

    def mixed(ref, q, both):
        diag = jnp.concatenate(
            [jnp.concatenate([ref[2 * q], zero], 1), jnp.concatenate([zero, ref[2 * q + 1]], 1)], 0)
        return lax.dot_general(
            diag, both, (((0,), (0,)), ((), ())), preferred_element_type=jnp.float32).astype(jnp.bfloat16)

    for q in range(couples):
        at = slice(q * TILE, (q + 1) * TILE)
        both = coef[2 * q:2 * q + 2].reshape(2 * rank, rows)
        coef2[:, at] = both.T
        wei2[at, :] = mixed(dens, q, both)
        tri2[at, :] = mixed(amps, q, ints[2 * q:2 * q + 2].reshape(2 * rank, rows))

    def mask(row, value):
        return jnp.where(ids[row] == value, 1.0, 0.0).astype(jnp.bfloat16)

    half_rows = rows // 2

    def place(dst, dst_row, src, src_row, count, first, value):
        m0, m1 = mask(first, value), mask(first + 1, value)
        for r in range(0, count, SUB):
            a = src[pl.ds(pl.multiple_of(src_row + r, SUB), SUB), :]
            b = src[pl.ds(pl.multiple_of(src_row + half_rows + r, SUB), SUB), :]
            dst[pl.ds(pl.multiple_of(dst_row + r, SUB), SUB), :] = a * m0 + b * m1

    for count, base, offset, y_first in ((na, 0, 0, 0), (nb, 4 * na, na, 1), (nc, 4 * nab, nab, 0)):

        def lhs_unit(n, carry, count=count, base=base, offset=offset, y_first=y_first):
            pieces = count // SUB
            half, ij, t = n // (4 * pieces), (n // pieces) % 4, n % pieces
            i, j = ij // 2, ij % 2
            si, sj = (j, i) if y_first else (i, j)
            cc = (1 - half) * (1 - c) + half * c
            xx = (1 - si) * (1 - x) + si * x
            yy = (1 - sj) * (1 - y) + sj * y
            row = ((yy * 2 + xx) * 2 + cc) * shard + offset + t * SUB
            place(lhs, half * (4 * shard) + base + (ij * pieces + t) * SUB, coef2,
                  row % half_rows, SUB, 0, row // half_rows)
            return carry

        lax.fori_loop(0, 8 * (count // SUB), lhs_unit, 0)

    chunk_of = ((1 - z1) * 2 + 1 - z0, (1 - z1) * 2 + z0, z1 * 2 + 1 - z0, z)

    def build(step):
        k = chunk_of[step]
        virt_first = 3 * (k // 2) + k % 2

        def switch(label, value):
            return jnp.full((rank, TILE), jnp.where(label == value, 1.0, 0.0), jnp.float32).astype(jnp.bfloat16)

        def one_pair(n, carry):
            at = pl.ds(pl.multiple_of(n * rank, rank), rank)
            for src, blocks, labels, start, base in (
                (tri2, ABPO, [aux[h, n] * ABPO + off[h, n] for h in range(2)], k * ABPO, 0),
                (wei2, 2, [pao[h, n] for h in range(2)], virt_first, ABPO),
            ):
                low_part, high_part = src[at, 0:TILE], src[at, TILE:2 * TILE]
                for j in range(blocks):
                    rhs[step % 2, at, (base + j) * TILE:(base + j + 1) * TILE] = (
                        low_part * switch(labels[0], start + j) + high_part * switch(labels[1], start + j))
            return carry

        lax.fori_loop(0, pairs, one_pair, 0, unroll=2)

    n_rows = 4 * shard
    wide = 2 * TILE

    def product(step, half, dst, kind):
        left = lhs.at[pl.ds(half * n_rows, n_rows)]

        def body(t, carry):
            at = pl.ds(pl.multiple_of(t * wide, wide), wide)
            dst[:, at] = lax.dot_general(
                left[...], rhs[step % 2, :, at], (((1,), (0,)), ((), ())),
                preferred_element_type=jnp.float32).astype(kind)
            return carry

        lax.fori_loop(0, lanes // wide, body, 0)

    f32, bf16 = jnp.float32, jnp.bfloat16
    stage1 = {}
    stage2 = {}
    zcopy = {}
    to_b, to_c = 4 * na, 4 * nab
    a_dev, b_dev = (xdev, ydev), (ydev, xdev)

    def first(step):
        stage1[step, "c"].wait_recv()

        def summed(lo, hi):
            return own[lo:hi, :] + c_recv[step, lo:hi, :].astype(f32)

        def quarters(base, count):
            order = (0, 1, 2, 3) if step % 2 == 0 else (0, 2, 1, 3)
            return [summed(base + n * count, base + (n + 1) * count) for n in order]

        a_parts, b_parts = quarters(0, na), quarters(to_b, nb)
        ax_send[step, 0:na] = a_parts[0].astype(bf16)
        ax_send[step, na:2 * na] = a_parts[1].astype(bf16)
        stage1[step, "a"] = send(ax_send.at[step], ax_recv.at[step], a_dev[step % 2])
        by_send[step, 0:nb] = b_parts[0].astype(bf16)
        by_send[step, nb:2 * nb] = b_parts[1].astype(bf16)
        stage1[step, "b"] = send(by_send.at[step], by_recv.at[step], b_dev[step % 2])
        if step in (0, 2):
            cz_send[step // 2] = summed(to_c, to_c + 4 * nc).astype(bf16)
            zcopy["c", step] = send(cz_send.at[step // 2], cz_recv.at[step // 2], z0dev)
        else:
            ck[step // 2] = summed(to_c, to_c + 4 * nc)
        mid = 2 * na
        keep1[step, 0:na] = a_parts[2]
        keep1[step, na:mid] = a_parts[3]
        keep1[step, mid:mid + nb] = b_parts[2]
        keep1[step, mid + nb:2 * nab] = b_parts[3]

    def second(step):
        stage1[step, "a"].wait_recv()
        ay_send[step] = (keep1[step, 0:na] + ax_recv[step, 0:na].astype(f32)).astype(bf16)
        stage2[step, "a"] = send(ay_send.at[step], ay_recv.at[step], b_dev[step % 2])
        stage1[step, "b"].wait_recv()
        mid = 2 * na
        bx_send[step] = (keep1[step, mid:mid + nb] + by_recv[step, 0:nb].astype(f32)).astype(bf16)
        stage2[step, "b"] = send(bx_send.at[step], bx_recv.at[step], a_dev[step % 2])
        keep2[step, 0:na] = keep1[step, na:mid] + ax_recv[step, na:mid].astype(f32)
        keep2[step, na:nab] = keep1[step, mid + nb:2 * nab] + by_recv[step, nb:2 * nb].astype(f32)

    def third_sum(step, lo, hi):
        got = ay_recv if lo == 0 else bx_recv
        return keep2[step, lo:hi] + got[step].astype(f32)

    halves = ((0, na), (na, nab))

    def third(step):
        stage2[step, "a"].wait_recv()
        stage2[step, "b"].wait_recv()
        if step in (0, 2):
            for lo, hi in halves:
                pz_send[step // 2, lo:hi] = third_sum(step, lo, hi).astype(bf16)
            zcopy["p", step] = send(pz_send.at[step // 2], pz_recv.at[step // 2], z0dev)
        elif step == 1:
            zcopy["p", 0].wait_recv()
            for lo, hi in halves:
                pw_send[lo:hi] = (third_sum(step, lo, hi) + pz_recv[0, lo:hi].astype(f32)).astype(bf16)
            zcopy["p", 1] = send(pw_send, pw_recv, z1dev)
        else:
            zcopy["p", 1].wait_recv()
            zcopy["p", 2].wait_recv()
            for lo, hi in halves:
                out[lo:hi] = third_sum(step, lo, hi) + pz_recv[1, lo:hi].astype(f32) + pw_recv[lo:hi].astype(f32)

    def c_across():
        zcopy["c", 0].wait_recv()
        cw_send[...] = (ck[0] + cz_recv[0].astype(f32)).astype(bf16)
        zcopy["c", 1] = send(cw_send, cw_recv, z1dev)

    def c_sum(lo, hi):
        return ck[1, lo:hi] + cz_recv[1, lo:hi].astype(f32) + cw_recv[lo:hi].astype(f32)

    def c_x():
        zcopy["c", 2].wait_recv()
        zcopy["c", 1].wait_recv()
        cx_send[...] = c_sum(0, 2 * nc).astype(bf16)
        zcopy["cx"] = send(cx_send, cx_recv, xdev)
        ckx[...] = c_sum(2 * nc, 4 * nc)

    def c_y():
        zcopy["cx"].wait_recv()
        cy_send[...] = (ckx[0:nc] + cx_recv[0:nc].astype(f32)).astype(bf16)
        zcopy["cy"] = send(cy_send, cy_recv, ydev)
        ckx[nc:2 * nc] = ckx[nc:2 * nc] + cx_recv[nc:2 * nc].astype(f32)

    build(0)
    for step in range(4):
        product(step, 0, c_send.at[step], bf16)
        if step == 0:
            pl.semaphore_wait(barrier, 5)
        stage1[step, "c"] = send(c_send.at[step], c_recv.at[step], core)
        product(step, 1, own, f32)
        if step == 2:
            c_across()
        if step < 3:
            build(step + 1)
        first(step)
        if step >= 2:
            second(step - 2)
    third(0)
    second(2)
    c_x()
    second(3)
    third(1)
    c_y()
    third(2)
    third(3)
    zcopy["cy"].wait_recv()
    out[nab:shard] = ckx[nc:2 * nc] + cy_recv[...].astype(f32)
    aux_lanes = gamma.shape[1]
    gamma[...] = out[0:shard, 0:aux_lanes] * scale
    out[shard:] = jnp.zeros((out.shape[0] - shard, lanes), f32)
    turned[...] = out[:, aux_lanes:].T * scale
    strip = virt.shape[0]
    virt[...] = turned[pl.ds(pl.multiple_of(z0 * (turned.shape[0] - strip), 8), strip), 0:shard]
    for copy in started:
        copy.wait_send()


COPIES = 4 + 8 + 8 + 2 + 1 + 2 + 1 + 2


def by_kernel(integrals, amplitudes, pno_density, pno_coef, pao_blocks, aux_slice, aux_offset):
    n_pair = lax.axis_size("pair")
    n_aux = lax.axis_size("aux")
    pairs, rows, rank = pno_coef.shape
    block = rows // pao_blocks.shape[1]
    ao_count = NBLK * block
    shard = ao_count // n_pair
    na, nb, nc = group_rows(shard)
    nab = na + nb
    aux_lanes = ABPO * block
    lanes = aux_lanes + 2 * block
    width = pairs * rank
    scale = 1.0 / math.sqrt(pairs * n_pair)
    vmem = pl.BlockSpec(memory_space=pltpu.VMEM)
    smem = pl.BlockSpec(memory_space=pltpu.SMEM)

    def half(*dims):
        return pltpu.VMEM(dims + (lanes,), jnp.bfloat16)

    def full(*dims):
        return pltpu.VMEM(dims + (lanes,), jnp.float32)

    gamma, virt = pl.pallas_call(
        functools.partial(kernel, scale),
        out_shape=[
            jax.ShapeDtypeStruct((shard, aux_lanes), jnp.float32),
            jax.ShapeDtypeStruct((ao_count // n_aux, shard), jnp.float32),
        ],
        in_specs=[vmem] * 4 + [smem] * 3,
        out_specs=[vmem] * 2,
        scratch_shapes=[
            full(TILE),
            pltpu.VMEM((rows, width), jnp.bfloat16),
            pltpu.VMEM((width, rows), jnp.bfloat16),
            pltpu.VMEM((width, rows), jnp.bfloat16),
            pltpu.VMEM((2, SUB, width), jnp.int32),
            pltpu.VMEM((8 * shard, width), jnp.bfloat16),
            pltpu.VMEM((2, width, lanes), jnp.bfloat16),
            full(4 * shard),
            half(4, 4 * shard), half(4, 4 * shard),
            half(4, 2 * na), half(4, 2 * na), half(4, na), half(4, na),
            half(4, 2 * nb), half(4, 2 * nb), half(4, nb), half(4, nb),
            full(4, 2 * nab), full(4, nab),
            half(2, 4 * nc), half(2, 4 * nc), half(4 * nc), half(4 * nc), full(2, 4 * nc),
            half(2, nab), half(2, nab), half(nab), half(nab),
            half(2 * nc), half(2 * nc), half(nc), half(nc), full(2 * nc),
            pltpu.VMEM((2 * block, TILE), jnp.float32),
            pltpu.SemaphoreType.DMA((COPIES,)),
            pltpu.SemaphoreType.DMA((COPIES,)),
        ],
        compiler_params=pltpu.CompilerParams(
            collective_id=0, has_side_effects=True, vmem_limit_bytes=60 * 1024 * 1024),
    )(integrals.swapaxes(1, 2), amplitudes, pno_density, pno_coef.swapaxes(1, 2),
      pao_blocks.T, aux_slice.T, aux_offset.T)
    return gamma.T, virt


def on_device(*args):
    pairs, rows, rank = args[3].shape
    fits = lax.axis_size("pair") == 8 and lax.axis_size("aux") == 4 and pairs % 2 == 0 and 2 * rank == TILE
    fits = fits and rows == 2 * TILE and args[0].shape[1] == 2 * TILE
    return by_kernel(*args) if fits else by_collectives(*args)


def solution(mesh):
    in_specs = (
        P(("pair", "aux"), None, None),
        P(("pair", "aux"), None, None),
        P(("pair", "aux"), None, None),
        P(("pair", "aux"), None, None),
        P(("pair", "aux"), None),
        P(("pair", "aux"), None),
        P(("pair", "aux"), None),
    )
    out_specs = (P("aux", "pair"), P("aux", "pair"))
    return jax.shard_map(
        on_device, mesh=mesh, in_specs=in_specs, out_specs=out_specs, check_vma=False
    )
```
